32 devices in a mesh: lon: 8 (over y, x, core), dp: 4 (over z).
Axes of the slice: x: 2, y: 2, z: 4, core: 2. Of those that a mesh axis runs over, the one named last changes fastest.
Arguments:
- inputs: bfloat16 [4, 32, 384, 256], P('dp', None, 'lon'), may hold values from -6 to 6
- pre_act: bfloat16 [4, 32, 384, 256], P('dp', None, 'lon'), may hold values from -6 to 6
- cotangent: bfloat16 [4, 32, 384, 256], P('dp', None, 'lon'), may hold values from -6 to 6
- first_weight: bfloat16 [2304, 256], replicated, may hold values from -0.125 to 0.125
- second_weight: bfloat16 [2304, 256], replicated, may hold values from -0.125 to 0.125
Outputs:
- input_gradient_array: bfloat16 [4, 32, 384, 256], P('dp', None, 'lon')
- first_weight_gradient: float32 [589824], P(('lon', 'dp'))
- second_weight_gradient: float32 [589824], P(('lon', 'dp'))
The draws below stay inside these ranges and needn't reach their ends.
All inputs are finite; a program needn't handle non-finite values.
Results may differ from the reference program's by a relative error of at most 0.0049.
Values may be sent and summed in bfloat16 or wider, within the bound.
A program may use at most 64 MiB of HBM per device.

```python
import jax
import jax.numpy as jnp

C = 256
FIRST_SPREAD = 12
SECOND_SPREAD = 18
LAT = 32
NLON = 384
SAMPLES = 4


def shard_levels(stream_key, shape, split, least, largest):
    def one(axis_at, blocks):
        steps = jax.random.uniform(jax.random.fold_in(jax.random.fold_in(stream_key, 6), axis_at), (blocks,), jnp.float32, least / len(split), largest / len(split))
        return jnp.repeat(jnp.exp(steps), shape[axis_at] // blocks).reshape((-1,) + (1,) * (len(shape) - axis_at - 1))

    level = one(*split[0])
    for cut in split[1:]:
        level = level * one(*cut)
    return level


def bell_draw(key, extent, scale, bound, cuts=(), held_as=jnp.bfloat16):
    result = scale * jax.random.normal(key, extent, jnp.float32)
    if cuts:
        result = result * shard_levels(key, extent, cuts, -0.22, 0.18)
    return jnp.clip(result, -bound, bound).astype(held_as)


def setup_inputs(seed: int = 0) -> dict:
    seeds = jax.random.split(jax.random.key(seed), 6)
    return {
        "inputs": bell_draw(seeds[0], (SAMPLES, LAT, NLON, C), 1.0, 6.0, ((0, 4), (2, 8))),
        "pre_act": bell_draw(seeds[1], (SAMPLES, LAT, NLON, C), 1.0, 6.0, ((0, 4), (2, 8))),
        "cotangent": bell_draw(seeds[2], (SAMPLES, LAT, NLON, C), 1.0, 6.0, ((0, 4), (2, 8))),
        "first_weight": bell_draw(seeds[3], (9 * C, C), (9 * C) ** -0.5, 0.125),
        "second_weight": bell_draw(seeds[4], (9 * C, C), (9 * C) ** -0.5, 0.125),
    }


def lat_move(values, offset):
    rows = values.shape[1]
    if abs(offset) >= rows:
        return jnp.zeros_like(values)
    if offset == 0:
        return values
    blank = jnp.zeros_like(values[:, :abs(offset)])
    if offset > 0:
        return jnp.concatenate([values[:, offset:], blank], axis=1)
    return jnp.concatenate([blank, values[:, :rows + offset]], axis=1)


def shifted(values, dilation, tap, direction):
    lat_off = direction * (tap // 3 - 1) * dilation
    lon_off = direction * (tap % 3 - 1) * dilation
    return lat_move(jnp.roll(values, -lon_off, axis=2), lat_off)


def kernel_weight_gradient(source, dilation, upstream):
    chans = upstream.shape[3]
    flat_up = upstream.reshape(-1, chans)
    blocks = []
    for tap in range(9):
        moved = shifted(source, dilation, tap, 1).reshape(-1, source.shape[3])
        blocks.append(jnp.dot(moved.T, flat_up, preferred_element_type=jnp.float32))
    return jnp.concatenate(blocks, axis=0)


def gradient_wrt_input(upstream, dilation, weights):
    chans = weights.shape[1]
    total = jnp.zeros((upstream.shape[0] * upstream.shape[1] * upstream.shape[2], weights.shape[1]), jnp.float32)
    for tap in range(9):
        moved = shifted(upstream, dilation, tap, -1).reshape(-1, chans)
        block = weights[tap * chans:(tap + 1) * chans]
        total = total + jnp.dot(moved, block.T, preferred_element_type=jnp.float32)
    return total.reshape(upstream.shape)


def reference(inputs, pre_act, cotangent, first_weight, second_weight):
    norm_factor = float(SAMPLES * LAT * NLON) ** -0.5
    hidden_activation = jnp.maximum(pre_act, jnp.zeros_like(pre_act))
    second_weight_gradient = (kernel_weight_gradient(hidden_activation, SECOND_SPREAD, cotangent) * norm_factor).reshape(-1)
    hidden_gradient = gradient_wrt_input(cotangent, SECOND_SPREAD, second_weight)
    partial_gradient = jnp.where(pre_act > 0, hidden_gradient, jnp.float32(0.0)).astype(jnp.bfloat16)
    first_weight_gradient = (kernel_weight_gradient(inputs, FIRST_SPREAD, partial_gradient) * norm_factor).reshape(-1)
    input_gradient_array = gradient_wrt_input(partial_gradient, FIRST_SPREAD, first_weight).astype(jnp.bfloat16)
    return input_gradient_array, first_weight_gradient, second_weight_gradient
```

```python
import functools

import jax
import jax.numpy as jnp
from jax import lax
from jax.experimental import pallas as pl
from jax.experimental.pallas import tpu as pltpu
from jax.sharding import PartitionSpec as P

FIRST_SPREAD = 12
SECOND_SPREAD = 18
MESH = pl.DeviceIdType.MESH
F32 = jnp.float32
BF16 = jnp.bfloat16
LANE_SLOT = (0, 2, 1)


def row_span(rows, dilation, r):
    if r == 0:
        return 0, rows - dilation, dilation
    if r == 1:
        return 0, rows, 0
    return dilation, rows, 0


def dot_nt(a, b):
    return lax.dot_general(a, b, (((1,), (1,)), ((), ())), preferred_element_type=F32)


def dot_tn(a, b):
    return lax.dot_general(a, b, (((0,), (0,)), ((), ())), preferred_element_type=F32)


def flat(v):
    return v.reshape(-1, v.shape[-1])


def kernel(nl, nd, scatter, norm, *refs):
    inp, pre, cot, w1, w2 = refs[:5]
    ig_out, g1_out, g2_out = refs[5:8]
    (cot_v, pre_v, inp_v, lg_v, ig_v, w1_v, w2_v, side2, side1, acc) = refs[8:18]
    (in_sem, w1_sem, w2_sem, out_sem) = refs[18:22]
    (s2_lo, s2_hi, r2_lo, r2_hi, s1_lo, s1_hi, r1_lo, r1_hi, hs_sem, hr_sem) = refs[22:32]
    if scatter:
        (dw1, dw2, ps1, ps2, pr1, pr2, as1, as2, ar1, ar2) = refs[32:42]
        (p_ssem, p_rsem, a_ssem, a_rsem) = refs[42:46]
    else:
        dw1, dw2 = g1_out, g2_out

    rows, cols, ch = cot_v.shape
    me_l, me_d = lax.axis_index("lon"), lax.axis_index("dp")
    left, right = lax.rem(me_l + nl - 1, nl), lax.rem(me_l + 1, nl)
    half = nl // 2
    slots = half * nd
    core = lax.rem(me_l, 2)
    my_slot = (me_l // 2) * nd + me_d

    def slot_device(slot):
        return (2 * (slot // nd) + core, lax.rem(slot, nd))

    load_cot = pltpu.make_async_copy(cot.at[0], cot_v, in_sem.at[0])
    load_pre = pltpu.make_async_copy(pre.at[0], pre_v, in_sem.at[1])
    load_inp = pltpu.make_async_copy(inp.at[0], inp_v, in_sem.at[2])

    def weight_loads(w, w_v, sem):
        return [
            pltpu.make_async_copy(
                w.at[pl.ds(k * ch, ch)],
                w_v.at[k // 3, :, pl.ds(LANE_SLOT.index(k % 3) * ch, ch)],
                sem.at[k],
            )
            for k in range(9)
        ]

    load_w2 = weight_loads(w2, w2_v, w2_sem)
    load_w1 = weight_loads(w1, w1_v, w1_sem)
    load_cot.start()
    for c in load_w2:
        c.start()
    load_pre.start()
    load_inp.start()
    for c in load_w1:
        c.start()

    barrier = pltpu.get_barrier_semaphore()
    for other in (left, right):
        pl.semaphore_signal(barrier, inc=1, device_id=(other, me_d), device_id_type=MESH)
    greeted = 2
    if scatter:

        def greet(t, _):
            pl.semaphore_signal(
                barrier,
                inc=1,
                device_id=slot_device(lax.rem(my_slot + t, slots)),
                device_id_type=MESH,
            )
            return 0

        lax.fori_loop(1, slots, greet, 0)
        greeted += slots - 1

    def halo_copies(lo, hi, from_right, from_left, base):
        return (
            pltpu.make_async_remote_copy(
                src_ref=lo, dst_ref=from_right, send_sem=hs_sem.at[base],
                recv_sem=hr_sem.at[base], device_id=(left, me_d), device_id_type=MESH,
            ),
            pltpu.make_async_remote_copy(
                src_ref=hi, dst_ref=from_left, send_sem=hs_sem.at[base + 1],
                recv_sem=hr_sem.at[base + 1], device_id=(right, me_d), device_id_type=MESH,
            ),
        )

    def pack(src, lo, hi, d):
        for p in range(rows):
            lo[p * d : (p + 1) * d, :] = src[p, 0:d, :]
            hi[p * d : (p + 1) * d, :] = src[p, cols - d : cols, :]

    def side_inner(src, side, d):
        side[:, 0 : cols - d, 0:ch] = src[:, d:cols, :]
        side[:, d:cols, ch : 2 * ch] = src[:, 0 : cols - d, :]

    def side_edges(side, from_right, from_left, d):
        side[:, cols - d : cols, 0:ch] = from_right[...].reshape(rows, d, ch)
        side[:, 0:d, ch : 2 * ch] = from_left[...].reshape(rows, d, ch)

    def input_terms(src, lanes, w_v, wl, d, fresh):
        for r in (1, 0, 2):
            lo, hi, first = row_span(rows, d, r)
            term = dot_nt(
                flat(src[first : first + hi - lo, :, 0:lanes]), w_v[r, :, wl : wl + lanes]
            )
            if fresh and r == 1:
                acc[...] = term
            else:
                acc[lo * cols : hi * cols, :] += term

    def weight_terms(x, src, lanes, dw, taps, d):
        for r in range(3):
            lo, hi, first = row_span(rows, d, r)
            term = dot_tn(flat(x[lo:hi]), flat(src[first : first + hi - lo, :, 0:lanes]))
            for at, c in enumerate(taps):
                k = 3 * r + c
                value = term[:, at * ch : (at + 1) * ch]
                dw[k * ch : (k + 1) * ch, :] = value if scatter else value * norm

    if scatter:
        depth = dw1.shape[0] // (nl * nd)

        def chunk_rows(slot, parity):
            l, d = 2 * (slot // nd) + parity, lax.rem(slot, nd)
            return pl.ds(pl.multiple_of((l * nd + d) * depth, 8), depth)

        def pair_copy(ps, pr, at):
            partner = me_l + 1 - 2 * core
            return pltpu.make_async_remote_copy(
                src_ref=ps, dst_ref=pr, send_sem=p_ssem.at[at], recv_sem=p_rsem.at[at],
                device_id=(partner, me_d), device_id_type=MESH,
            )

        def pair_pack(dw, ps):
            def one(s, _):
                v = dw[chunk_rows(s, 1 - core), :].astype(BF16)
                ps[s, 0:depth, :] = v[:, : ch // 2]
                ps[s, depth : 2 * depth, :] = v[:, ch // 2 :]
                return 0

            lax.fori_loop(0, slots, one, 0)

        def chip_sum(dw, pr, s):
            v = dw[chunk_rows(s, core), :]
            return (
                v[:, : ch // 2] + pr[s, 0:depth, :].astype(F32),
                v[:, ch // 2 :] + pr[s, depth : 2 * depth, :].astype(F32),
            )

        def spread_copy(a_s, a_r, at, t):
            slot = lax.rem(my_slot + t, slots)
            return pltpu.make_async_remote_copy(
                src_ref=a_s.at[slot], dst_ref=a_r.at[t], send_sem=a_ssem.at[at, t],
                recv_sem=a_rsem.at[at, t], device_id=slot_device(slot), device_id_type=MESH,
            )

        def spread(dw, pr, a_s, a_r, at):
            def fill(s, _):
                lo, hi = chip_sum(dw, pr, s)
                a_s[s, 0:depth, :] = lo.astype(BF16)
                a_s[s, depth : 2 * depth, :] = hi.astype(BF16)
                return 0

            lax.fori_loop(0, slots, fill, 0)

            def send(t, _):
                spread_copy(a_s, a_r, at, t).start()
                return 0

            lax.fori_loop(1, slots, send, 0)

        def gather_sum(dw, pr, a_s, a_r, at, out):
            def add(t, total):
                spread_copy(a_s, a_r, at, t).wait()
                return (
                    total[0] + a_r[t, 0:depth, :].astype(F32),
                    total[1] + a_r[t, depth : 2 * depth, :].astype(F32),
                )

            lo, hi = lax.fori_loop(1, slots, add, chip_sum(dw, pr, my_slot))
            out[pl.ds(0, depth, stride=2), :] = lo * norm
            out[pl.ds(1, depth, stride=2), :] = hi * norm

    load_cot.wait()
    pack(cot_v, s2_lo, s2_hi, SECOND_SPREAD)
    pl.semaphore_wait(barrier, greeted)
    halo2 = halo_copies(s2_lo, s2_hi, r2_lo, r2_hi, 0)
    for c in halo2:
        c.start()
    side_inner(cot_v, side2, SECOND_SPREAD)
    for c in load_w2:
        c.wait()
    input_terms(cot_v, ch, w2_v, 2 * ch, SECOND_SPREAD, True)
    load_pre.wait()
    zero = jnp.zeros((), BF16)
    pre_v[...] = jnp.maximum(pre_v[...], zero)
    weight_terms(pre_v, cot_v, ch, dw2, (1,), SECOND_SPREAD)
    for c in halo2:
        c.wait()
    side_edges(side2, r2_lo, r2_hi, SECOND_SPREAD)
    input_terms(side2, 2 * ch, w2_v, 0, SECOND_SPREAD, False)
    grad = jnp.where(flat(pre_v[...]) > 0, acc[...], F32(0.0)).astype(BF16)
    lg_v[...] = grad.reshape(rows, cols, ch)
    pack(lg_v, s1_lo, s1_hi, FIRST_SPREAD)
    halo1 = halo_copies(s1_lo, s1_hi, r1_lo, r1_hi, 2)
    for c in halo1:
        c.start()
    weight_terms(pre_v, side2, 2 * ch, dw2, (0, 2), SECOND_SPREAD)
    if scatter:
        pair_pack(dw2, ps2)
        pair2 = pair_copy(ps2, pr2, 0)
        pair2.start()

    load_inp.wait()
    side_inner(lg_v, side1, FIRST_SPREAD)
    weight_terms(inp_v, lg_v, ch, dw1, (1,), FIRST_SPREAD)
    if scatter:
        pair2.wait()
        spread(dw2, pr2, as2, ar2, 0)
    for c in halo1:
        c.wait()
    side_edges(side1, r1_lo, r1_hi, FIRST_SPREAD)
    weight_terms(inp_v, side1, 2 * ch, dw1, (0, 2), FIRST_SPREAD)
    if scatter:
        pair_pack(dw1, ps1)
        pair1 = pair_copy(ps1, pr1, 1)
        pair1.start()
    for c in load_w1:
        c.wait()
    input_terms(lg_v, ch, w1_v, 2 * ch, FIRST_SPREAD, True)
    if scatter:
        pair1.wait()
        spread(dw1, pr1, as1, ar1, 1)
    input_terms(side1, 2 * ch, w1_v, 0, FIRST_SPREAD, False)
    ig_v[...] = acc[...].astype(BF16).reshape(rows, cols, ch)
    store = pltpu.make_async_copy(ig_v, ig_out.at[0], out_sem)
    store.start()
    if scatter:
        gather_sum(dw2, pr2, as2, ar2, 0, g2_out)
        gather_sum(dw1, pr1, as1, ar1, 1, g1_out)
    store.wait()


def local(nl, nd, inputs, pre_act, cotangent, first_weight, second_weight):
    _, rows, cols, ch = inputs.shape
    taps_rows = first_weight.shape[0]
    norm = float(rows * cols * nl * inputs.shape[0] * nd) ** -0.5
    devices = nl * nd
    depth = taps_rows // devices
    scatter = nl % 2 == 0 and taps_rows % devices == 0 and depth % 8 == 0
    slots = devices // 2
    vm = pltpu.VMEM
    dma = pltpu.SemaphoreType.DMA
    field = vm((rows, cols, ch), BF16)
    edge2 = vm((rows * SECOND_SPREAD, ch), BF16)
    edge1 = vm((rows * FIRST_SPREAD, ch), BF16)
    weights = vm((3, ch, 3 * ch), BF16)
    side = vm((rows, cols, 2 * ch), BF16)
    scratch = [field] * 5 + [weights] * 2 + [side] * 2 + [vm((rows * cols, ch), F32)]
    scratch += [dma((3,)), dma((9,)), dma((9,)), dma]
    scratch += [edge2] * 4 + [edge1] * 4 + [dma((4,)), dma((4,))]
    if scatter:
        pieces = vm((slots, 2 * depth, ch // 2), BF16)
        scratch += [vm((taps_rows, ch), F32)] * 2 + [pieces] * 8
        scratch += [dma((2,)), dma((2,)), dma((2, slots)), dma((2, slots))]
        grad_shape = (2 * depth, ch // 2)
    else:
        grad_shape = (taps_rows, ch)
    any_spec = pl.BlockSpec(memory_space=pl.ANY)
    vmem_spec = pl.BlockSpec(memory_space=pltpu.VMEM)
    ig, g1, g2 = pl.pallas_call(
        functools.partial(kernel, nl, nd, scatter, norm),
        out_shape=(
            jax.ShapeDtypeStruct(inputs.shape, BF16),
            jax.ShapeDtypeStruct(grad_shape, F32),
            jax.ShapeDtypeStruct(grad_shape, F32),
        ),
        in_specs=[any_spec] * 5,
        out_specs=(any_spec, vmem_spec, vmem_spec),
        scratch_shapes=scratch,
        compiler_params=pltpu.CompilerParams(
            collective_id=0, has_side_effects=True, vmem_limit_bytes=48 * 1024 * 1024
        ),
        name="conv_backward",
    )(inputs, pre_act, cotangent, first_weight, second_weight)
    g1, g2 = g1.reshape(-1), g2.reshape(-1)
    if not scatter:
        g1, g2 = (lax.psum_scatter(g, "lon", scatter_dimension=0, tiled=True) for g in (g1, g2))
        g1, g2 = (lax.psum_scatter(g, "dp", scatter_dimension=0, tiled=True) for g in (g1, g2))
    return ig, g1, g2


def solution(mesh):
    in_specs = (
        P("dp", None, "lon", None),
        P("dp", None, "lon", None),
        P("dp", None, "lon", None),
        P(),
        P(),
    )
    out_specs = (P("dp", None, "lon", None), P(("lon", "dp")), P(("lon", "dp")))
    step = functools.partial(local, mesh.shape["lon"], mesh.shape["dp"])
    return jax.shard_map(step, mesh=mesh, in_specs=in_specs, out_specs=out_specs, check_vma=False)
```

```python
import functools

import jax
import jax.numpy as jnp
from jax import lax
from jax.experimental import pallas as pl
from jax.experimental.pallas import tpu as pltpu
from jax.sharding import PartitionSpec as P

FIRST_SPREAD = 12
SECOND_SPREAD = 18
MESH = pl.DeviceIdType.MESH
F32 = jnp.float32
BF16 = jnp.bfloat16
LANE_SLOT = (0, 2, 1)


def row_span(rows, dilation, r):
    if r == 0:
        return 0, rows - dilation, dilation
    if r == 1:
        return 0, rows, 0
    return dilation, rows, 0


def dot_nt(a, b):
    return lax.dot_general(a, b, (((1,), (1,)), ((), ())), preferred_element_type=F32)


def dot_tn(a, b):
    return lax.dot_general(a, b, (((0,), (0,)), ((), ())), preferred_element_type=F32)


def flat(v):
    return v.reshape(-1, v.shape[-1])


def kernel(nl, nd, scatter, norm, *refs):
    inp, pre, cot, w1, w2 = refs[:5]
    ig_out, g1_out, g2_out = refs[5:8]
    (cot_v, pre_v, inp_v, lg_v, ig_v, w1_v, w2_v, side2, side1, acc) = refs[8:18]
    (in_sem, w1_sem, w2_sem, out_sem) = refs[18:22]
    (s2_lo, s2_hi, r2_lo, r2_hi, s1_lo, s1_hi, r1_lo, r1_hi, hs_sem, hr_sem) = refs[22:32]
    if scatter:
        (dw1, dw2, ps1, ps2, pr1, pr2, as1, as2, ar1, ar2) = refs[32:42]
        (zs1, zs2, zr1, zr2, p_ssem, p_rsem, a_ssem, a_rsem, z_ssem, z_rsem) = refs[42:52]
    else:
        dw1, dw2 = g1_out, g2_out

    rows, cols, ch = cot_v.shape
    me_l, me_d = lax.axis_index("lon"), lax.axis_index("dp")
    left, right = lax.rem(me_l + nl - 1, nl), lax.rem(me_l + 1, nl)
    half = nl // 2
    slots = half * nd
    core = lax.rem(me_l, 2)

    my_chip = me_l // 2

    def plane_device(t):
        return (2 * lax.rem(my_chip + t, half) + core, me_d)

    def depth_device(u):
        return (me_l, lax.rem(me_d + u, nd))

    load_cot = pltpu.make_async_copy(cot.at[0], cot_v, in_sem.at[0])
    load_pre = pltpu.make_async_copy(pre.at[0], pre_v, in_sem.at[1])
    load_inp = pltpu.make_async_copy(inp.at[0], inp_v, in_sem.at[2])

    def weight_loads(w, w_v, sem):
        return [
            pltpu.make_async_copy(
                w.at[pl.ds(k * ch, ch)],
                w_v.at[k // 3, :, pl.ds(LANE_SLOT.index(k % 3) * ch, ch)],
                sem.at[k],
            )
            for k in range(9)
        ]

    load_w2 = weight_loads(w2, w2_v, w2_sem)
    load_w1 = weight_loads(w1, w1_v, w1_sem)
    load_cot.start()
    for c in load_w2:
        c.start()
    load_pre.start()
    load_inp.start()
    for c in load_w1:
        c.start()

    barrier = pltpu.get_barrier_semaphore()
    for other in (left, right):
        pl.semaphore_signal(barrier, inc=1, device_id=(other, me_d), device_id_type=MESH)
    greeted = 2
    if scatter:
        for t in range(1, half):
            pl.semaphore_signal(barrier, inc=1, device_id=plane_device(t), device_id_type=MESH)
        for u in range(1, nd):
            pl.semaphore_signal(barrier, inc=1, device_id=depth_device(u), device_id_type=MESH)
        greeted += half - 1 + nd - 1

    def halo_copies(lo, hi, from_right, from_left, base):
        return (
            pltpu.make_async_remote_copy(
                src_ref=lo, dst_ref=from_right, send_sem=hs_sem.at[base],
                recv_sem=hr_sem.at[base], device_id=(left, me_d), device_id_type=MESH,
            ),
            pltpu.make_async_remote_copy(
                src_ref=hi, dst_ref=from_left, send_sem=hs_sem.at[base + 1],
                recv_sem=hr_sem.at[base + 1], device_id=(right, me_d), device_id_type=MESH,
            ),
        )

    def pack(src, lo, hi, d):
        for p in range(rows):
            lo[p * d : (p + 1) * d, :] = src[p, 0:d, :]
            hi[p * d : (p + 1) * d, :] = src[p, cols - d : cols, :]

    def side_inner(src, side, d):
        side[:, 0 : cols - d, 0:ch] = src[:, d:cols, :]
        side[:, d:cols, ch : 2 * ch] = src[:, 0 : cols - d, :]

    def side_edges(side, from_right, from_left, d):
        side[:, cols - d : cols, 0:ch] = from_right[...].reshape(rows, d, ch)
        side[:, 0:d, ch : 2 * ch] = from_left[...].reshape(rows, d, ch)

    def input_terms(src, lanes, w_v, wl, d, fresh):
        for r in (1, 0, 2):
            lo, hi, first = row_span(rows, d, r)
            term = dot_nt(
                flat(src[first : first + hi - lo, :, 0:lanes]), w_v[r, :, wl : wl + lanes]
            )
            if fresh and r == 1:
                acc[...] = term
            else:
                acc[lo * cols : hi * cols, :] += term

    def weight_terms(x, src, lanes, dw, taps, d):
        for r in range(3):
            lo, hi, first = row_span(rows, d, r)
            term = dot_tn(flat(x[lo:hi]), flat(src[first : first + hi - lo, :, 0:lanes]))
            for at, c in enumerate(taps):
                k = 3 * r + c
                value = term[:, at * ch : (at + 1) * ch]
                dw[k * ch : (k + 1) * ch, :] = value if scatter else value * norm

    if scatter:
        depth = dw1.shape[0] // (nl * nd)
        plane_order = (*range(1, half), 0)

        def chunk_rows(slot, parity):
            l, d = 2 * (slot // nd) + parity, lax.rem(slot, nd)
            return pl.ds(pl.multiple_of((l * nd + d) * depth, 8), depth)

        def pair_copy(ps, pr, at, t):
            part = pl.ds(lax.rem(my_chip + t, half) * nd, nd)
            return pltpu.make_async_remote_copy(
                src_ref=ps.at[part], dst_ref=pr.at[part],
                send_sem=p_ssem.at[at, t], recv_sem=p_rsem.at[at, t],
                device_id=(me_l + 1 - 2 * core, me_d), device_id_type=MESH,
            )

        def pair_send(dw, ps, pr, at):
            for t in plane_order:
                for d in range(nd):
                    s = lax.rem(my_chip + t, half) * nd + d
                    v = dw[chunk_rows(s, 1 - core), :].astype(BF16)
                    ps[s, 0:depth, :] = v[:, : ch // 2]
                    ps[s, depth : 2 * depth, :] = v[:, ch // 2 :]
                pair_copy(ps, pr, at, t).start()

        def chip_sum(dw, pr, s):
            v = dw[chunk_rows(s, core), :]
            return (
                v[:, : ch // 2] + pr[s, 0:depth, :].astype(F32),
                v[:, ch // 2 :] + pr[s, depth : 2 * depth, :].astype(F32),
            )

        def plane_copy(a_s, a_r, at, t):
            chip = lax.rem(my_chip + t, half)
            return pltpu.make_async_remote_copy(
                src_ref=a_s.at[pl.ds(chip * nd, nd)], dst_ref=a_r.at[pl.ds(t * nd, nd)],
                send_sem=a_ssem.at[at, t], recv_sem=a_rsem.at[at, t],
                device_id=plane_device(t), device_id_type=MESH,
            )

        def depth_copy(z_s, z_r, at, u):
            return pltpu.make_async_remote_copy(
                src_ref=z_s.at[lax.rem(me_d + u, nd)], dst_ref=z_r.at[u],
                send_sem=z_ssem.at[at, u], recv_sem=z_rsem.at[at, u],
                device_id=depth_device(u), device_id_type=MESH,
            )

        def spread(dw, ps, pr, a_s, a_r, at):
            for t in plane_order:
                pair_copy(ps, pr, at, t).wait()
                if t == 0:
                    continue
                for d in range(nd):
                    s = lax.rem(my_chip + t, half) * nd + d
                    lo, hi = chip_sum(dw, pr, s)
                    a_s[s, 0:depth, :] = lo.astype(BF16)
                    a_s[s, depth : 2 * depth, :] = hi.astype(BF16)
                plane_copy(a_s, a_r, at, t).start()

        def plane_sum(dw, pr, a_r, d):
            lo, hi = chip_sum(dw, pr, my_chip * nd + d)
            for t in range(1, half):
                lo += a_r[t * nd + d, 0:depth, :].astype(F32)
                hi += a_r[t * nd + d, depth : 2 * depth, :].astype(F32)
            return lo, hi

        def across(dw, pr, a_s, a_r, z_s, z_r, at):
            for t in range(1, half):
                plane_copy(a_s, a_r, at, t).wait()

            for u in range(1, nd):
                d = lax.rem(me_d + u, nd)
                lo, hi = plane_sum(dw, pr, a_r, d)
                z_s[d, 0:depth, :] = lo.astype(BF16)
                z_s[d, depth : 2 * depth, :] = hi.astype(BF16)
                depth_copy(z_s, z_r, at, u).start()

        def gather_sum(dw, pr, a_r, z_s, z_r, at, out):
            lo, hi = plane_sum(dw, pr, a_r, me_d)
            for u in range(1, nd):
                depth_copy(z_s, z_r, at, u).wait()
                lo += z_r[u, 0:depth, :].astype(F32)
                hi += z_r[u, depth : 2 * depth, :].astype(F32)
            out[pl.ds(0, depth, stride=2), :] = lo * norm
            out[pl.ds(1, depth, stride=2), :] = hi * norm

    load_cot.wait()
    pack(cot_v, s2_lo, s2_hi, SECOND_SPREAD)
    pl.semaphore_wait(barrier, greeted)
    halo2 = halo_copies(s2_lo, s2_hi, r2_lo, r2_hi, 0)
    for c in halo2:
        c.start()
    side_inner(cot_v, side2, SECOND_SPREAD)
    for c in load_w2:
        c.wait()
    input_terms(cot_v, ch, w2_v, 2 * ch, SECOND_SPREAD, True)
    load_pre.wait()
    zero = jnp.zeros((), BF16)
    pre_v[...] = jnp.maximum(pre_v[...], zero)
    weight_terms(pre_v, cot_v, ch, dw2, (1,), SECOND_SPREAD)
    for c in halo2:
        c.wait()
    side_edges(side2, r2_lo, r2_hi, SECOND_SPREAD)
    input_terms(side2, 2 * ch, w2_v, 0, SECOND_SPREAD, False)
    grad = jnp.where(flat(pre_v[...]) > 0, acc[...], F32(0.0)).astype(BF16)
    lg_v[...] = grad.reshape(rows, cols, ch)
    pack(lg_v, s1_lo, s1_hi, FIRST_SPREAD)
    halo1 = halo_copies(s1_lo, s1_hi, r1_lo, r1_hi, 2)
    for c in halo1:
        c.start()
    weight_terms(pre_v, side2, 2 * ch, dw2, (0, 2), SECOND_SPREAD)
    if scatter:
        pair_send(dw2, ps2, pr2, 0)

    load_inp.wait()
    side_inner(lg_v, side1, FIRST_SPREAD)
    weight_terms(inp_v, lg_v, ch, dw1, (1,), FIRST_SPREAD)
    if scatter:
        spread(dw2, ps2, pr2, as2, ar2, 0)
    for c in halo1:
        c.wait()
    side_edges(side1, r1_lo, r1_hi, FIRST_SPREAD)
    weight_terms(inp_v, side1, 2 * ch, dw1, (0, 2), FIRST_SPREAD)
    if scatter:
        pair_send(dw1, ps1, pr1, 1)
    for c in load_w1:
        c.wait()
    input_terms(lg_v, ch, w1_v, 2 * ch, FIRST_SPREAD, True)
    if scatter:
        spread(dw1, ps1, pr1, as1, ar1, 1)
        across(dw2, pr2, as2, ar2, zs2, zr2, 0)
    input_terms(side1, 2 * ch, w1_v, 0, FIRST_SPREAD, False)
    ig_v[...] = acc[...].astype(BF16).reshape(rows, cols, ch)
    store = pltpu.make_async_copy(ig_v, ig_out.at[0], out_sem)
    store.start()
    if scatter:
        across(dw1, pr1, as1, ar1, zs1, zr1, 1)
        gather_sum(dw2, pr2, ar2, zs2, zr2, 0, g2_out)
        gather_sum(dw1, pr1, ar1, zs1, zr1, 1, g1_out)
    store.wait()


def local(nl, nd, inputs, pre_act, cotangent, first_weight, second_weight):
    _, rows, cols, ch = inputs.shape
    taps_rows = first_weight.shape[0]
    norm = float(rows * cols * nl * inputs.shape[0] * nd) ** -0.5
    devices = nl * nd
    depth = taps_rows // devices
    scatter = nl % 2 == 0 and taps_rows % devices == 0 and depth % 8 == 0
    slots = devices // 2
    vm = pltpu.VMEM
    dma = pltpu.SemaphoreType.DMA
    field = vm((rows, cols, ch), BF16)
    edge2 = vm((rows * SECOND_SPREAD, ch), BF16)
    edge1 = vm((rows * FIRST_SPREAD, ch), BF16)
    weights = vm((3, ch, 3 * ch), BF16)
    side = vm((rows, cols, 2 * ch), BF16)
    scratch = [field] * 5 + [weights] * 2 + [side] * 2 + [vm((rows * cols, ch), F32)]
    scratch += [dma((3,)), dma((9,)), dma((9,)), dma]
    scratch += [edge2] * 4 + [edge1] * 4 + [dma((4,)), dma((4,))]
    if scatter:
        pieces = vm((slots, 2 * depth, ch // 2), BF16)
        scratch += [vm((taps_rows, ch), F32)] * 2 + [pieces] * 8
        scratch += [vm((nd, 2 * depth, ch // 2), BF16)] * 4
        scratch += [dma((2, nl // 2))] * 4 + [dma((2, nd))] * 2
        grad_shape = (2 * depth, ch // 2)
    else:
        grad_shape = (taps_rows, ch)
    any_spec = pl.BlockSpec(memory_space=pl.ANY)
    vmem_spec = pl.BlockSpec(memory_space=pltpu.VMEM)
    ig, g1, g2 = pl.pallas_call(
        functools.partial(kernel, nl, nd, scatter, norm),
        out_shape=(
            jax.ShapeDtypeStruct(inputs.shape, BF16),
            jax.ShapeDtypeStruct(grad_shape, F32),
            jax.ShapeDtypeStruct(grad_shape, F32),
        ),
        in_specs=[any_spec] * 5,
        out_specs=(any_spec, vmem_spec, vmem_spec),
        scratch_shapes=scratch,
        compiler_params=pltpu.CompilerParams(
            collective_id=0, has_side_effects=True, vmem_limit_bytes=62 * 1024 * 1024
        ),
        name="conv_backward",
    )(inputs, pre_act, cotangent, first_weight, second_weight)
    g1, g2 = g1.reshape(-1), g2.reshape(-1)
    if not scatter:
        g1, g2 = (lax.psum_scatter(g, "lon", scatter_dimension=0, tiled=True) for g in (g1, g2))
        g1, g2 = (lax.psum_scatter(g, "dp", scatter_dimension=0, tiled=True) for g in (g1, g2))
    return ig, g1, g2


def solution(mesh):
    in_specs = (
        P("dp", None, "lon", None),
        P("dp", None, "lon", None),
        P("dp", None, "lon", None),
        P(),
        P(),
    )
    out_specs = (P("dp", None, "lon", None), P(("lon", "dp")), P(("lon", "dp")))
    step = functools.partial(local, mesh.shape["lon"], mesh.shape["dp"])
    return jax.shard_map(step, mesh=mesh, in_specs=in_specs, out_specs=out_specs, check_vma=False)
```

```python
import functools

import jax
import jax.numpy as jnp
from jax import lax
from jax.experimental import pallas as pl
from jax.experimental.pallas import tpu as pltpu
from jax.sharding import PartitionSpec as P

FIRST_SPREAD = 12
SECOND_SPREAD = 18
MESH = pl.DeviceIdType.MESH
F32 = jnp.float32
BF16 = jnp.bfloat16
LANE_SLOT = (0, 2, 1)


def row_span(rows, dilation, r):
    if r == 0:
        return 0, rows - dilation, dilation
    if r == 1:
        return 0, rows, 0
    return dilation, rows, 0


def dot_nt(a, b):
    return lax.dot_general(a, b, (((1,), (1,)), ((), ())), preferred_element_type=F32)


def dot_tn(a, b):
    return lax.dot_general(a, b, (((0,), (0,)), ((), ())), preferred_element_type=F32)


def flat(v):
    return v.reshape(-1, v.shape[-1])


def kernel(nl, nd, scatter, norm, *refs):
    inp, pre, cot, w1, w2 = refs[:5]
    ig_out, g1_out, g2_out = refs[5:8]
    (cot_v, pre_v, inp_v, lg_v, ig_v, w1_v, w2_v, side2, side1, acc) = refs[8:18]
    (in_sem, w1_sem, w2_sem, out_sem) = refs[18:22]
    (s2_lo, s2_hi, r2_lo, r2_hi, s1_lo, s1_hi, r1_lo, r1_hi, hs_sem, hr_sem) = refs[22:32]
    if scatter:
        (dw1, dw2, ps1, ps2, pr1, pr2, as1, as2, ar1, ar2) = refs[32:42]
        (zs1, zs2, zr1, zr2, p_ssem, p_rsem, a_ssem, a_rsem, z_ssem, z_rsem) = refs[42:52]
    else:
        dw1, dw2 = g1_out, g2_out

    rows, cols, ch = cot_v.shape
    me_l, me_d = lax.axis_index("lon"), lax.axis_index("dp")
    left, right = lax.rem(me_l + nl - 1, nl), lax.rem(me_l + 1, nl)
    half = nl // 2
    slots = half * nd
    core = lax.rem(me_l, 2)

    my_chip = me_l // 2

    def plane_device(t):
        return (2 * lax.rem(my_chip + t, half) + core, me_d)

    def depth_device(u):
        return (me_l, lax.rem(me_d + u, nd))

    load_cot = pltpu.make_async_copy(cot.at[0], cot_v, in_sem.at[0])
    load_pre = pltpu.make_async_copy(pre.at[0], pre_v, in_sem.at[1])
    load_inp = pltpu.make_async_copy(inp.at[0], inp_v, in_sem.at[2])

    def weight_loads(w, w_v, sem):
        return [
            pltpu.make_async_copy(
                w.at[pl.ds(k * ch, ch)],
                w_v.at[k // 3, :, pl.ds(LANE_SLOT.index(k % 3) * ch, ch)],
                sem.at[k],
            )
            for k in range(9)
        ]

    load_w2 = weight_loads(w2, w2_v, w2_sem)
    load_w1 = weight_loads(w1, w1_v, w1_sem)
    load_cot.start()
    for c in load_w2:
        c.start()
    load_pre.start()
    load_inp.start()
    for c in load_w1:
        c.start()

    barrier = pltpu.get_barrier_semaphore()
    for other in (left, right):
        pl.semaphore_signal(barrier, inc=1, device_id=(other, me_d), device_id_type=MESH)
    greeted = 2
    if scatter:
        for t in range(1, half):
            pl.semaphore_signal(barrier, inc=1, device_id=plane_device(t), device_id_type=MESH)
        for u in range(1, nd):
            pl.semaphore_signal(barrier, inc=1, device_id=depth_device(u), device_id_type=MESH)
        greeted += half - 1 + nd - 1

    def halo_copies(lo, hi, from_right, from_left, base):
        return (
            pltpu.make_async_remote_copy(
                src_ref=lo, dst_ref=from_right, send_sem=hs_sem.at[base],
                recv_sem=hr_sem.at[base], device_id=(left, me_d), device_id_type=MESH,
            ),
            pltpu.make_async_remote_copy(
                src_ref=hi, dst_ref=from_left, send_sem=hs_sem.at[base + 1],
                recv_sem=hr_sem.at[base + 1], device_id=(right, me_d), device_id_type=MESH,
            ),
        )

    def pack(src, lo, hi, d):
        for p in range(rows):
            lo[p * d : (p + 1) * d, :] = src[p, 0:d, :]
            hi[p * d : (p + 1) * d, :] = src[p, cols - d : cols, :]

    def side_inner(src, side, d):
        side[:, 0 : cols - d, 0:ch] = src[:, d:cols, :]
        side[:, d:cols, ch : 2 * ch] = src[:, 0 : cols - d, :]

    def side_edges(side, from_right, from_left, d):
        side[:, cols - d : cols, 0:ch] = from_right[...].reshape(rows, d, ch)
        side[:, 0:d, ch : 2 * ch] = from_left[...].reshape(rows, d, ch)

    def input_terms(src, lanes, w_v, wl, d, fresh):
        for r in (1, 0, 2):
            lo, hi, first = row_span(rows, d, r)
            term = dot_nt(
                flat(src[first : first + hi - lo, :, 0:lanes]), w_v[r, :, wl : wl + lanes]
            )
            if fresh and r == 1:
                acc[...] = term
            else:
                acc[lo * cols : hi * cols, :] += term

    def weight_terms(x, src, lanes, dw, taps, d):
        for r in range(3):
            lo, hi, first = row_span(rows, d, r)
            term = dot_tn(flat(x[lo:hi]), flat(src[first : first + hi - lo, :, 0:lanes]))
            for at, c in enumerate(taps):
                k = 3 * r + c
                value = term[:, at * ch : (at + 1) * ch]
                dw[k * ch : (k + 1) * ch, :] = value if scatter else value * norm

    if scatter:
        depth = dw1.shape[0] // (nl * nd)
        plane_order = (*range(1, half, 2), *range(2, half, 2), 0)

        def chunk_rows(slot, parity):
            l, d = 2 * (slot // nd) + parity, lax.rem(slot, nd)
            return pl.ds(pl.multiple_of((l * nd + d) * depth, 8), depth)

        def pair_copy(ps, pr, at, t):
            part = pl.ds(lax.rem(my_chip + t, half) * nd, nd)
            return pltpu.make_async_remote_copy(
                src_ref=ps.at[part], dst_ref=pr.at[part],
                send_sem=p_ssem.at[at, t], recv_sem=p_rsem.at[at, t],
                device_id=(me_l + 1 - 2 * core, me_d), device_id_type=MESH,
            )

        def pair_send(dw, ps, pr, at):
            for t in plane_order:
                for d in range(nd):
                    s = lax.rem(my_chip + t, half) * nd + d
                    v = dw[chunk_rows(s, 1 - core), :].astype(BF16)
                    ps[s, 0:depth, :] = v[:, : ch // 2]
                    ps[s, depth : 2 * depth, :] = v[:, ch // 2 :]
                pair_copy(ps, pr, at, t).start()

        def chip_sum(dw, pr, s):
            v = dw[chunk_rows(s, core), :]
            return (
                v[:, : ch // 2] + pr[s, 0:depth, :].astype(F32),
                v[:, ch // 2 :] + pr[s, depth : 2 * depth, :].astype(F32),
            )

        def plane_copy(a_s, a_r, at, t):
            chip = lax.rem(my_chip + t, half)
            return pltpu.make_async_remote_copy(
                src_ref=a_s.at[pl.ds(chip * nd, nd)], dst_ref=a_r.at[pl.ds(t * nd, nd)],
                send_sem=a_ssem.at[at, t], recv_sem=a_rsem.at[at, t],
                device_id=plane_device(t), device_id_type=MESH,
            )

        def depth_copy(z_s, z_r, at, u):
            return pltpu.make_async_remote_copy(
                src_ref=z_s.at[lax.rem(me_d + u, nd)], dst_ref=z_r.at[u],
                send_sem=z_ssem.at[at, u], recv_sem=z_rsem.at[at, u],
                device_id=depth_device(u), device_id_type=MESH,
            )

        def spread(dw, ps, pr, a_s, a_r, at):
            for t in plane_order:
                pair_copy(ps, pr, at, t).wait()
                if t == 0:
                    continue
                for d in range(nd):
                    s = lax.rem(my_chip + t, half) * nd + d
                    lo, hi = chip_sum(dw, pr, s)
                    a_s[s, 0:depth, :] = lo.astype(BF16)
                    a_s[s, depth : 2 * depth, :] = hi.astype(BF16)
                plane_copy(a_s, a_r, at, t).start()

        def plane_sum(dw, pr, a_r, d):
            lo, hi = chip_sum(dw, pr, my_chip * nd + d)
            for t in range(1, half):
                lo += a_r[t * nd + d, 0:depth, :].astype(F32)
                hi += a_r[t * nd + d, depth : 2 * depth, :].astype(F32)
            return lo, hi

        def across(dw, pr, a_s, a_r, z_s, z_r, at):
            for t in range(1, half):
                plane_copy(a_s, a_r, at, t).wait()

            for u in range(1, nd):
                d = lax.rem(me_d + u, nd)
                lo, hi = plane_sum(dw, pr, a_r, d)
                z_s[d, 0:depth, :] = lo.astype(BF16)
                z_s[d, depth : 2 * depth, :] = hi.astype(BF16)
                depth_copy(z_s, z_r, at, u).start()

        def gather_sum(dw, pr, a_r, z_s, z_r, at, out):
            lo, hi = plane_sum(dw, pr, a_r, me_d)
            for u in range(1, nd):
                depth_copy(z_s, z_r, at, u).wait()
                lo += z_r[u, 0:depth, :].astype(F32)
                hi += z_r[u, depth : 2 * depth, :].astype(F32)
            out[pl.ds(0, depth, stride=2), :] = lo * norm
            out[pl.ds(1, depth, stride=2), :] = hi * norm

    load_cot.wait()
    pack(cot_v, s2_lo, s2_hi, SECOND_SPREAD)
    pl.semaphore_wait(barrier, greeted)
    halo2 = halo_copies(s2_lo, s2_hi, r2_lo, r2_hi, 0)
    for c in halo2:
        c.start()
    side_inner(cot_v, side2, SECOND_SPREAD)
    for c in load_w2:
        c.wait()
    input_terms(cot_v, ch, w2_v, 2 * ch, SECOND_SPREAD, True)
    load_pre.wait()
    zero = jnp.zeros((), BF16)
    pre_v[...] = jnp.maximum(pre_v[...], zero)
    weight_terms(pre_v, cot_v, ch, dw2, (1,), SECOND_SPREAD)
    for c in halo2:
        c.wait()
    side_edges(side2, r2_lo, r2_hi, SECOND_SPREAD)
    input_terms(side2, 2 * ch, w2_v, 0, SECOND_SPREAD, False)
    grad = jnp.where(flat(pre_v[...]) > 0, acc[...], F32(0.0)).astype(BF16)
    lg_v[...] = grad.reshape(rows, cols, ch)
    halo1 = halo_copies(s1_lo, s1_hi, r1_lo, r1_hi, 2)
    for p in range(rows):
        s1_lo[p * FIRST_SPREAD : (p + 1) * FIRST_SPREAD, :] = lg_v[p, 0:FIRST_SPREAD, :]
    halo1[0].start()
    for p in range(rows):
        s1_hi[p * FIRST_SPREAD : (p + 1) * FIRST_SPREAD, :] = lg_v[p, cols - FIRST_SPREAD : cols, :]
    halo1[1].start()
    weight_terms(pre_v, side2, 2 * ch, dw2, (0, 2), SECOND_SPREAD)
    if scatter:
        pair_send(dw2, ps2, pr2, 0)

    load_inp.wait()
    side_inner(lg_v, side1, FIRST_SPREAD)
    weight_terms(inp_v, lg_v, ch, dw1, (1,), FIRST_SPREAD)
    if scatter:
        spread(dw2, ps2, pr2, as2, ar2, 0)
    for c in halo1:
        c.wait()
    side_edges(side1, r1_lo, r1_hi, FIRST_SPREAD)
    weight_terms(inp_v, side1, 2 * ch, dw1, (0, 2), FIRST_SPREAD)
    if scatter:
        pair_send(dw1, ps1, pr1, 1)
    for c in load_w1:
        c.wait()
    input_terms(lg_v, ch, w1_v, 2 * ch, FIRST_SPREAD, True)
    if scatter:
        spread(dw1, ps1, pr1, as1, ar1, 1)
        across(dw2, pr2, as2, ar2, zs2, zr2, 0)
    input_terms(side1, 2 * ch, w1_v, 0, FIRST_SPREAD, False)
    ig_v[...] = acc[...].astype(BF16).reshape(rows, cols, ch)
    store = pltpu.make_async_copy(ig_v, ig_out.at[0], out_sem)
    store.start()
    if scatter:
        across(dw1, pr1, as1, ar1, zs1, zr1, 1)
        gather_sum(dw2, pr2, ar2, zs2, zr2, 0, g2_out)
        gather_sum(dw1, pr1, ar1, zs1, zr1, 1, g1_out)
    store.wait()


def local(nl, nd, inputs, pre_act, cotangent, first_weight, second_weight):
    _, rows, cols, ch = inputs.shape
    taps_rows = first_weight.shape[0]
    norm = float(rows * cols * nl * inputs.shape[0] * nd) ** -0.5
    devices = nl * nd
    depth = taps_rows // devices
    scatter = nl % 2 == 0 and taps_rows % devices == 0 and depth % 8 == 0
    slots = devices // 2
    vm = pltpu.VMEM
    dma = pltpu.SemaphoreType.DMA
    field = vm((rows, cols, ch), BF16)
    edge2 = vm((rows * SECOND_SPREAD, ch), BF16)
    edge1 = vm((rows * FIRST_SPREAD, ch), BF16)
    weights = vm((3, ch, 3 * ch), BF16)
    side = vm((rows, cols, 2 * ch), BF16)
    scratch = [field] * 5 + [weights] * 2 + [side] * 2 + [vm((rows * cols, ch), F32)]
    scratch += [dma((3,)), dma((9,)), dma((9,)), dma]
    scratch += [edge2] * 4 + [edge1] * 4 + [dma((4,)), dma((4,))]
    if scatter:
        pieces = vm((slots, 2 * depth, ch // 2), BF16)
        scratch += [vm((taps_rows, ch), F32)] * 2 + [pieces] * 8
        scratch += [vm((nd, 2 * depth, ch // 2), BF16)] * 4
        scratch += [dma((2, nl // 2))] * 4 + [dma((2, nd))] * 2
        grad_shape = (2 * depth, ch // 2)
    else:
        grad_shape = (taps_rows, ch)
    any_spec = pl.BlockSpec(memory_space=pl.ANY)
    vmem_spec = pl.BlockSpec(memory_space=pltpu.VMEM)
    ig, g1, g2 = pl.pallas_call(
        functools.partial(kernel, nl, nd, scatter, norm),
        out_shape=(
            jax.ShapeDtypeStruct(inputs.shape, BF16),
            jax.ShapeDtypeStruct(grad_shape, F32),
            jax.ShapeDtypeStruct(grad_shape, F32),
        ),
        in_specs=[any_spec] * 5,
        out_specs=(any_spec, vmem_spec, vmem_spec),
        scratch_shapes=scratch,
        compiler_params=pltpu.CompilerParams(
            collective_id=0, has_side_effects=True, vmem_limit_bytes=62 * 1024 * 1024
        ),
        name="conv_backward",
    )(inputs, pre_act, cotangent, first_weight, second_weight)
    g1, g2 = g1.reshape(-1), g2.reshape(-1)
    if not scatter:
        g1, g2 = (lax.psum_scatter(g, "lon", scatter_dimension=0, tiled=True) for g in (g1, g2))
        g1, g2 = (lax.psum_scatter(g, "dp", scatter_dimension=0, tiled=True) for g in (g1, g2))
    return ig, g1, g2


def solution(mesh):
    in_specs = (
        P("dp", None, "lon", None),
        P("dp", None, "lon", None),
        P("dp", None, "lon", None),
        P(),
        P(),
    )
    out_specs = (P("dp", None, "lon", None), P(("lon", "dp")), P(("lon", "dp")))
    step = functools.partial(local, mesh.shape["lon"], mesh.shape["dp"])
    return jax.shard_map(step, mesh=mesh, in_specs=in_specs, out_specs=out_specs, check_vma=False)
```
